32 devices in a mesh: seq: 16 (over z, y, x), ch: 2 (over core).
Axes of the slice: x: 2, y: 2, z: 4, core: 2. Of those that a mesh axis runs over, the one named last changes fastest.
Arguments:
- tokens: bfloat16 [2048, 8192], P('seq', 'ch'), may hold values from -6 to 6
- query_in: bfloat16 [2048, 8192], P('seq', 'ch'), may hold values from -6 to 6
- key_in: bfloat16 [2048, 8192], P('seq', 'ch'), may hold values from -6 to 6
- proj_in: bfloat16 [8192, 1536], P('ch', 'seq'), may hold values from -0.0625 to 0.0625
- proj_out: bfloat16 [1536, 8192], P('seq', 'ch'), may hold values from -0.15625 to 0.15625
- short_taps: float32 [3, 7, 8192], P(None, None, 'ch'), may hold values from -2.4 to 2.4
- residues: float32 [16, 8192], P(None, 'ch'), may hold values from -1.8 to 1.8
- mode_rates: float32 [16, 8192], P(None, 'ch'), may hold values from 0.00024414062 to 0.03
- skip_gain: float32 [8192], P('ch'), may hold values from -3 to 3
Outputs:
- operator_out: bfloat16 [2048, 8192], P('seq', 'ch')
The draws below stay inside these ranges and needn't reach their ends.
All inputs are finite; a program needn't handle non-finite values.
Results may differ from the reference program's by a relative error of at most 0.0069.
Values may be sent and summed in bfloat16 or wider, within the bound.
A program may use at most 192 MiB of HBM per device.

```python
import math
import jax
import jax.numpy as jnp
from jax import lax

D = 8192
R = 1536
SHORT = 7
MODES = 16
SEQ = 2048


def steps_of(key, extent, cuts, low, top_value):
    gain, own = 1.0, jax.random.fold_in(key, 6)
    for axis_at, blocks in cuts:
        draws = jnp.exp(jax.random.uniform(jax.random.fold_in(own, axis_at), (blocks,), jnp.float32, low / len(cuts), top_value / len(cuts)))
        gain = gain * jnp.repeat(draws, extent[axis_at] // blocks).reshape([-1 if axis == axis_at else 1 for axis in range(len(extent))])
    return gain


def bell_draw(stream_key, shape, deviation, most, pieces=(), kind=jnp.bfloat16):
    entries = jax.random.normal(stream_key, shape, jnp.float32) * deviation
    if len(pieces) > 0:
        entries = steps_of(stream_key, shape, pieces, -0.22, 0.18) * entries
    return jnp.clip(entries, min=-most, max=most).astype(kind)


def setup_inputs(seed: int = 0) -> dict:
    key_list = jax.random.split(jax.random.key(seed), 10)
    return {
        "tokens": bell_draw(key_list[0], (SEQ, D), 1.0, 6.0, ((0, 16), (1, 2))),
        "query_in": bell_draw(key_list[1], (SEQ, D), 1.0, 6.0, ((0, 16), (1, 2))),
        "key_in": bell_draw(key_list[2], (SEQ, D), 1.0, 6.0, ((0, 16), (1, 2))),
        "proj_in": bell_draw(key_list[3], (D, R), D ** -0.5, 0.0625, ((0, 2), (1, 16))),
        "proj_out": bell_draw(key_list[4], (R, D), R ** -0.5, 0.15625, ((0, 16), (1, 2))),
        "short_taps": bell_draw(key_list[5], (3, SHORT, D), 0.4, 2.4, ((2, 2),), jnp.float32),
        "residues": bell_draw(key_list[6], (MODES, D), 0.3, 1.8, ((1, 2),), jnp.float32),
        "mode_rates": jnp.clip(jnp.exp(math.log(0.03) - 4.8112082 * jax.random.uniform(key_list[7], (MODES, D), jnp.float32) ** steps_of(key_list[7], (MODES, D), ((1, 2),), -0.2, 0.2)), 0.00024414062, 0.03),
        "skip_gain": bell_draw(key_list[8], (D,), 0.5, 3.0, ((0, 2),), jnp.float32),
    }


def causal_short(signal, filter_taps):
    margin_rows = filter_taps.shape[0] - 1
    length = signal.shape[0]
    padded = jnp.pad(signal, ((margin_rows, 0), (0, 0)))
    result = filter_taps[0] * padded[margin_rows:margin_rows + length]
    for offset in range(1, margin_rows + 1):
        result = result + filter_taps[offset] * padded[margin_rows - offset:margin_rows - offset + length]
    return result

def long_block(operands):
    mixed_block, residue_block, rate_block = operands
    positions = jnp.arange(SEQ).astype(jnp.float32)[:, None]
    impulse = jnp.zeros((SEQ, mixed_block.shape[1]), jnp.float32)
    for mode_index in range(MODES):
        impulse = impulse + residue_block[mode_index] * jnp.sqrt(rate_block[mode_index]) * jnp.exp(-rate_block[mode_index] * positions)
    spectrum = jnp.fft.rfft(mixed_block.astype(jnp.float32), n=2 * SEQ, axis=0) * jnp.fft.rfft(impulse, n=2 * SEQ, axis=0)
    return jnp.fft.irfft(spectrum, n=2 * SEQ, axis=0)[:SEQ].astype(jnp.bfloat16)

def reference(tokens, query_in, key_in, proj_in, proj_out, short_taps, residues, mode_rates, skip_gain):
    low_rank = jnp.dot(tokens, proj_in, preferred_element_type=jnp.float32).astype(jnp.bfloat16)
    value_proj = jnp.dot(low_rank, proj_out, preferred_element_type=jnp.float32).astype(jnp.bfloat16)
    query_short = causal_short(query_in.astype(jnp.float32), short_taps[0])
    key_short = causal_short(key_in.astype(jnp.float32), short_taps[1])
    value_short = causal_short(value_proj.astype(jnp.float32), short_taps[2])
    mixed = (key_short * value_short).astype(jnp.bfloat16)
    blocks = D // 128
    mixed_blocks = mixed.reshape(SEQ, blocks, 128).transpose(1, 0, 2)
    residue_blocks = residues.reshape(MODES, blocks, 128).transpose(1, 0, 2)
    rate_blocks = mode_rates.reshape(MODES, blocks, 128).transpose(1, 0, 2)
    convolved = lax.map(long_block, (mixed_blocks, residue_blocks, rate_blocks))
    convolved = convolved.transpose(1, 0, 2).reshape(SEQ, D)
    return (query_short * (convolved.astype(jnp.float32) + skip_gain * mixed.astype(jnp.float32))).astype(jnp.bfloat16)
```

```python
import functools

import jax
import jax.numpy as jnp
from jax import lax
from jax.experimental import pallas as pl
from jax.experimental.pallas import tpu as pltpu
from jax.sharding import PartitionSpec as P

MESH = pl.DeviceIdType.MESH
VMEM = pl.BlockSpec(memory_space=pltpu.VMEM)
ANY = pl.BlockSpec(memory_space=pl.ANY)
GROUP = 4


def flip(position):
    return position + (position // 2) * (1 - 2 * (position % 2))


def where_am_i():
    me = lax.axis_index("seq")
    return me // GROUP, me % GROUP


def device(plane, spot):
    return {"seq": plane * GROUP + spot}


def remote(source, target, sems, index, place):
    return pltpu.make_async_remote_copy(
        src_ref=source, dst_ref=target, send_sem=sems[0].at[index], recv_sem=sems[1].at[index],
        device_id=place, device_id_type=MESH,
    )


def greet(places):
    barrier = pltpu.get_barrier_semaphore()
    for place in places:
        pl.semaphore_signal(barrier, inc=1, device_id=place, device_id_type=MESH)
    pl.semaphore_wait(barrier, len(places))


class Ring:
    def __init__(self, own, slot, sems, base, mine, left, right, left_dev, right_dev):
        self.first = [
            remote(own(0), slot(mine, 0), sems, base, right_dev),
            remote(own(1), slot(mine, 1), sems, base + 1, left_dev),
            remote(own(1), slot(mine, 1), sems, base + 2, right_dev),
            remote(own(0), slot(mine, 0), sems, base + 3, left_dev),
        ]
        self.onward = [
            remote(slot(left, 0), slot(left, 0), sems, base + 4, right_dev),
            remote(slot(right, 1), slot(right, 1), sems, base + 5, left_dev),
        ]

    def start(self):
        for copy in self.first:
            copy.start()

    def relay(self):
        for arrived, onward in zip(self.first[:2], self.onward):
            arrived.wait_recv()
            onward.start()

    def finish(self):
        for copy in self.first[2:] + self.onward:
            copy.wait_recv()
        for copy in self.first + self.onward:
            copy.wait_send()


def rings():
    plane, spot = where_am_i()
    turn = flip(spot)
    left, right = flip((turn + GROUP - 1) % GROUP), flip((turn + 1) % GROUP)
    flat = (spot, left, right, device(plane, left), device(plane, right))
    below, above = (plane + GROUP - 1) % GROUP, (plane + 1) % GROUP
    tall = (plane, below, above, device(below, spot), device(above, spot))
    return plane, spot, flat, tall


def everyone(plane, spot, tall):
    return [device(plane, (spot + step) % GROUP) for step in range(1, GROUP)] + [tall[3], tall[4]]


def swap(piece, slot, sems, base, plane, spot):
    copies = []
    for step in range(1, GROUP):
        peer = (spot + step) % GROUP
        copies.append(remote(piece(peer), slot(spot), sems, base + step - 1, device(plane, peer)))
    return copies


def gather_first(tok, pin, pout, tok_all, pin_all, rows_late, rows_early, pieces, send, recv, local):
    plane, spot, flat, tall = rings()
    sems = (send, recv)
    width = pieces.shape[-1]
    greet(everyone(plane, spot, tall))

    def piece(peer):
        return pout.at[:, pl.ds(pl.multiple_of(peer * width, width), width)]

    half_tok, half_pin = tok.shape[0] // 2, pin.shape[0] // 2
    moved = swap(piece, lambda s: pieces.at[s], sems, 18, plane, spot)
    for copy in moved:
        copy.start()
    tokens_ring = Ring(
        lambda h: tok.at[pl.ds(h * half_tok, half_tok)],
        lambda s, h: tok_all.at[s, pl.ds(h * half_tok, half_tok)], sems, 0, *flat)
    pin_ring = Ring(
        lambda h: pin.at[pl.ds(h * half_pin, half_pin)],
        lambda s, h: pin_all.at[s, pl.ds(h * half_pin, half_pin)], sems, 6, *tall)
    tokens_ring.start()
    pin_ring.start()
    keep = [
        pltpu.make_async_copy(tok, tok_all.at[spot], local.at[0]),
        pltpu.make_async_copy(pin, pin_all.at[plane], local.at[1]),
        pltpu.make_async_copy(piece(spot), pieces.at[spot], local.at[2]),
    ]
    for copy in keep:
        copy.start()
    pin_ring.relay()
    keep[2].wait()
    for copy in moved:
        copy.wait_recv()
    rows_ring = Ring(
        lambda h: pieces.at[h], lambda s, h: rows_early.at[h, s], sems, 12, *tall)
    rows_ring.start()
    last = [
        pltpu.make_async_copy(pieces.at[pl.ds(2, 2)], rows_late, local.at[3]),
        pltpu.make_async_copy(pieces.at[0], rows_early.at[0, plane], local.at[4]),
        pltpu.make_async_copy(pieces.at[1], rows_early.at[1, plane], local.at[5]),
    ]
    for copy in last:
        copy.start()
    tokens_ring.relay()
    rows_ring.relay()
    pin_ring.finish()
    tokens_ring.finish()
    rows_ring.finish()
    for copy in moved:
        copy.wait_send()
    for copy in keep[:2] + last:
        copy.wait()


def gather_second(low, rows, key, low_all, rows_all, key_all, send, recv, local):
    plane, spot, flat, tall = rings()
    sems = (send, recv)
    width, ranks, half = key_all.shape[-1], low.shape[1], low.shape[0] // 2
    greet(everyone(plane, spot, tall))

    def columns(s):
        return pl.ds(pl.multiple_of(s * ranks, ranks), ranks)

    def piece(peer):
        return key.at[:, pl.ds(pl.multiple_of(peer * width, width), width)]

    low_ring = Ring(
        lambda h: low.at[pl.ds(h * half, half)],
        lambda s, h: low_all.at[pl.ds(h * half, half), columns(s)], sems, 0, *flat)
    rows_ring = Ring(lambda h: rows.at[h], lambda s, h: rows_all.at[h, s], sems, 6, *tall)
    moved = swap(piece, lambda s: key_all.at[s], sems, 12, plane, spot)
    low_ring.start()
    rows_ring.start()
    keep = [
        pltpu.make_async_copy(low, low_all.at[:, columns(spot)], local.at[0]),
        pltpu.make_async_copy(rows.at[0], rows_all.at[0, plane], local.at[1]),
        pltpu.make_async_copy(rows.at[1], rows_all.at[1, plane], local.at[2]),
        pltpu.make_async_copy(piece(spot), key_all.at[spot], local.at[3]),
    ]
    for copy in keep:
        copy.start()
    low_ring.relay()
    for copy in moved:
        copy.start()
    rows_ring.relay()
    low_ring.finish()
    rows_ring.finish()
    for copy in moved:
        copy.wait_recv()
    for copy in moved:
        copy.wait_send()
    for copy in keep:
        copy.wait()


def give_back(mine, out, send, recv, local):
    plane, spot = where_am_i()
    rows, width = out.shape[0], mine.shape[1]
    greet([device(plane, (spot + step) % GROUP) for step in range(1, GROUP)])

    def piece(peer):
        return mine.at[pl.ds(pl.multiple_of(peer * rows, rows), rows)]

    def slot(s):
        return out.at[:, pl.ds(pl.multiple_of(s * width, width), width)]

    moved = swap(piece, slot, (send, recv), 0, plane, spot)
    for copy in moved:
        copy.start()
    keep = pltpu.make_async_copy(piece(spot), slot(spot), local.at[0])
    keep.start()
    for copy in moved:
        copy.wait_recv()
    for copy in moved:
        copy.wait_send()
    keep.wait()


def talk(kernel, shapes, in_specs, scratch, copies, locals_, ident):
    one = not isinstance(shapes, (list, tuple))
    return pl.pallas_call(
        kernel,
        out_shape=shapes,
        in_specs=in_specs,
        out_specs=ANY if one else [ANY] * len(shapes),
        scratch_shapes=scratch + [
            pltpu.SemaphoreType.DMA((copies,)),
            pltpu.SemaphoreType.DMA((copies,)),
            pltpu.SemaphoreType.DMA((locals_,)),
        ],
        compiler_params=pltpu.CompilerParams(collective_id=ident, has_side_effects=True),
    )


def end_states(mixed, decay, spread, states):
    rows, (modes, tall, lanes) = mixed.shape[0], decay.shape

    @pl.loop(0, rows // 16)
    def _(block):
        start = pl.multiple_of(block * 16, 16)
        for column in range(tall):
            tile = mixed[pl.ds(start, 16), column * lanes:(column + 1) * lanes]
            spread[pl.ds(start * tall + column, 16, stride=tall), :] = tile.astype(jnp.float32)

    rates = [decay[mode] for mode in range(modes)]

    def step(at, held):
        for part in range(8):
            value = spread[pl.ds(pl.multiple_of((at * 8 + part) * tall, tall), tall), :]
            held = [h * r + value for h, r in zip(held, rates)]
        return held

    held = lax.fori_loop(0, rows // 8, step, [jnp.zeros((tall, lanes), jnp.float32)] * modes)
    for mode in range(modes):
        states[mode] = held[mode]


def run_states(spread, carried, decay, weight, skip, out, kept):
    modes, tall, lanes = decay.shape
    rows = out.shape[0]
    rates = [decay[mode] for mode in range(modes)]
    weights = [weight[mode] for mode in range(modes)]
    gain = skip[...]

    def step(at, held):
        for part in range(4):
            place = pl.ds(pl.multiple_of((at * 4 + part) * tall, tall), tall)
            value = spread[place, :]
            held = [h * r + value for h, r in zip(held, rates)]
            terms = [h * w for h, w in zip(held, weights)]
            while len(terms) > 1:
                terms = [a + b for a, b in zip(terms[::2], terms[1::2])]
            rounded = terms[0].astype(jnp.bfloat16).astype(jnp.float32)
            kept[place, :] = rounded + gain * value
        return held

    lax.fori_loop(0, rows // 4, step, [carried[mode] for mode in range(modes)])

    @pl.loop(0, rows // 16)
    def _(block):
        start = pl.multiple_of(block * 16, 16)
        for column in range(tall):
            tile = kept[pl.ds(start * tall + column, 16, stride=tall), :]
            out[pl.ds(start, 16), column * lanes:(column + 1) * lanes] = tile.astype(jnp.bfloat16)


def planes_device(
    tokens, query_in, key_in, proj_in, proj_out, short_taps, residues, mode_rates, skip_gain
):
    rows, channels = tokens.shape
    ranks = proj_in.shape[1]
    modes = residues.shape[0]
    margin_rows = short_taps.shape[1] - 1
    width, all_rows = channels // GROUP, rows * GROUP
    tall = width // 128
    half = jnp.bfloat16
    shape = jax.ShapeDtypeStruct
    plane, spot = where_am_i()
    query_previous = passed_along(query_in[rows - margin_rows:], "seq", 1)

    tok_all, pin_all, late, early = talk(
        gather_first,
        [shape((GROUP, rows, channels), half), shape((GROUP, ranks, channels), half),
         shape((2, ranks, width), half), shape((2, GROUP, ranks, width), half)],
        [VMEM] * 3, [pltpu.VMEM((GROUP, ranks, width), half)], 21, 6, 1,
    )(tokens, proj_in.T, proj_out)
    partial_value = lax.dot_general(
        tok_all.reshape(all_rows, channels), pin_all.reshape(GROUP * ranks, channels),
        (((1,), (1,)), ((), ())), preferred_element_type=jnp.float32)
    low_rank = lax.psum(partial_value, "ch").astype(half)
    low_all, rest, key_all = talk(
        gather_second,
        [shape((all_rows, GROUP * GROUP * ranks), half), shape((2, GROUP, ranks, width), half),
         shape((GROUP, rows, width), half)],
        [VMEM] * 3, [], 15, 4, 2,
    )(low_rank, late, key_in)
    factor = jnp.concatenate([early, rest], axis=0).reshape(GROUP * GROUP * ranks, width)
    value = jnp.dot(low_all, factor, preferred_element_type=jnp.float32).astype(half)
    key = key_all.reshape(all_rows, width)

    def mine(part):
        return lax.dynamic_slice_in_dim(part, spot * width, width, part.ndim - 1)

    taps, rates, weights = mine(short_taps[1:]), mine(mode_rates), mine(residues)
    edges = passed_along(
        jnp.stack([key[all_rows - margin_rows:], value[all_rows - margin_rows:]]), "seq", GROUP)
    mixed = (
        short_filter(edges[0], key, taps[0]) * short_filter(edges[1], value, taps[1])
    ).astype(half)
    tiles = (modes, tall, 128)
    weights = (weights * jnp.sqrt(rates)).reshape(tiles)
    rates = rates.reshape(tiles)
    decay = jnp.exp(-rates)
    spread, states = pl.pallas_call(
        end_states,
        out_shape=[shape((all_rows * tall, 128), jnp.float32), shape(tiles, jnp.float32)],
        in_specs=[VMEM] * 2, out_specs=[VMEM] * 2,
    )(mixed, decay)
    count = lax.axis_size("seq") // GROUP
    groups = [[at * GROUP + s for at in range(count)] for s in range(GROUP)]
    ends = lax.all_gather(states, "seq", axis_index_groups=groups)
    carried = jnp.zeros(tiles, jnp.float32)
    block = jnp.exp(-rates * all_rows)
    for at in range(count - 1):
        carried = jnp.where(at < plane, carried * block + ends[at], carried)
    mixed_out = pl.pallas_call(
        run_states,
        out_shape=shape((all_rows, width), half),
        in_specs=[VMEM] * 5, out_specs=VMEM,
        scratch_shapes=[pltpu.VMEM((all_rows * tall, 128), jnp.float32)],
    )(spread, carried, decay, weights, mine(skip_gain).reshape(tall, 128))
    given = talk(give_back, shape((rows, channels), half), [VMEM], [], 3, 1, 3)(mixed_out)
    query_short = short_filter(query_previous, query_in, short_taps[0])
    return (query_short * given.astype(jnp.float32)).astype(half)


precise = lax.Precision.HIGHEST


def carried_in(value, axis, join, neutral):
    count, mine = (lax.axis_size(axis), lax.axis_index(axis))
    pieces = jax.tree.map(lambda part: lax.all_gather(part, axis), value)
    total = jax.tree.map(
        lambda part, zero: jnp.full_like(part, 0) + jnp.asarray(zero, part.dtype), value, neutral
    )

    def turn(position, total):
        longer = join(total, jax.tree.map(lambda part: part[position], pieces))
        return jax.tree.map(lambda new, old: jnp.where(position < mine, new, old), longer, total)

    return lax.fori_loop(0, count - 1, turn, total)


def passed_along(value, axis, steps):
    count = lax.axis_size(axis)
    leading, last = (max(0, -steps), min(count, count - steps))
    return lax.ppermute(value, axis, [(source, source + steps) for source in range(leading, last)])


def short_filter(previous, current, filter_taps):
    margin_rows = filter_taps.shape[0] - 1
    length = current.shape[0]
    extended = jnp.concatenate([previous, current], axis=0).astype(jnp.float32)
    result = filter_taps[0] * extended[margin_rows : margin_rows + length]
    for offset in range(1, margin_rows + 1):
        result = (
            result
            + filter_taps[offset] * extended[margin_rows - offset : margin_rows - offset + length]
        )
    return result


def carry_states(earlier, later):
    return (earlier[0] * later[1] + later[0], earlier[1] * later[1])


def modal_convolve(mixed, residues, mode_rates):
    tok_rows = mixed.shape[0]
    signal = mixed.astype(jnp.float32)
    steps = jnp.arange(tok_rows, dtype=jnp.int32)
    lower = (steps[:, None] >= steps[None, :]).astype(jnp.float32)
    centred = (steps.astype(jnp.float32) - 0.5 * tok_rows)[:, None]
    local_total = jnp.zeros(signal.shape, jnp.float32)
    end_list = []
    for mode_index in range(residues.shape[0]):
        rate_mode = mode_rates[mode_index]
        weight = residues[mode_index] * jnp.sqrt(rate_mode)
        rising = jnp.exp(rate_mode * centred)
        falling = jnp.exp(-rate_mode * centred)
        running = falling * jnp.dot(lower, rising * signal, precision=precise)
        local_total = local_total + weight * running
        end_list.append(running[tok_rows - 1])
    end_states = jnp.stack(end_list)
    block_decay = jnp.exp(-mode_rates * tok_rows)
    identity = (jnp.zeros(end_states.shape, jnp.float32), jnp.ones(end_states.shape, jnp.float32))
    carried, _ = carried_in((end_states, block_decay), "seq", carry_states, identity)
    after = (steps.astype(jnp.float32) + 1.0)[:, None]
    for mode_index in range(residues.shape[0]):
        rate_mode = mode_rates[mode_index]
        weight = residues[mode_index] * jnp.sqrt(rate_mode)
        local_total = local_total + weight * carried[mode_index] * jnp.exp(-rate_mode * after)
    rounded = lax.optimization_barrier(local_total.astype(jnp.bfloat16))
    return rounded.astype(jnp.float32)


def per_device(
    tokens, query_in, key_in, proj_in, proj_out, short_taps, residues, mode_rates, skip_gain
):
    tok_rows = tokens.shape[0]
    margin_rows = short_taps.shape[1] - 1
    partial_value = jnp.dot(
        tokens,
        lax.all_gather(proj_in, "seq", axis=1, tiled=True),
        preferred_element_type=jnp.float32,
    )
    low_rank = lax.psum(partial_value, "ch").astype(jnp.bfloat16)
    value_full = jnp.dot(
        low_rank,
        lax.all_gather(proj_out, "seq", axis=0, tiled=True),
        preferred_element_type=jnp.float32,
    )
    value_proj = value_full.astype(jnp.bfloat16)
    edges = jnp.stack(
        [
            query_in[tok_rows - margin_rows :],
            key_in[tok_rows - margin_rows :],
            value_proj[tok_rows - margin_rows :],
        ]
    )
    arrived_edges = passed_along(edges, "seq", 1)
    query_previous = arrived_edges[0]
    key_previous = arrived_edges[1]
    value_previous = arrived_edges[2]
    query_short = short_filter(query_previous, query_in, short_taps[0])
    key_short = short_filter(key_previous, key_in, short_taps[1])
    value_short = short_filter(value_previous, value_proj, short_taps[2])
    mixed = (key_short * value_short).astype(jnp.bfloat16)
    convolved_tokens = modal_convolve(mixed, residues, mode_rates)
    return (query_short * (convolved_tokens + skip_gain * mixed.astype(jnp.float32))).astype(
        jnp.bfloat16
    )


def chosen(mesh):
    def run(*args):
        rows, channels = args[0].shape
        ranks = args[3].shape[1]
        square = mesh.shape["seq"] == GROUP * GROUP
        whole = channels % (GROUP * 1024) == 0 and ranks % 32 == 0 and rows % 32 == 0
        fits = (GROUP * ranks) % 128 == 0 and channels == GROUP * 1024
        return (planes_device if square and whole and fits else per_device)(*args)

    return run


def solution(mesh):
    placed = (
        P("seq", "ch"),
        P("seq", "ch"),
        P("seq", "ch"),
        P("ch", "seq"),
        P("seq", "ch"),
        P(None, None, "ch"),
        P(None, "ch"),
        P(None, "ch"),
        P("ch"),
    )
    return jax.shard_map(
        chosen(mesh), mesh=mesh, in_specs=placed, out_specs=P("seq", "ch"), check_vma=False
    )
```

```python
import functools

import jax
import jax.numpy as jnp
from jax import lax
from jax.experimental import pallas as pl
from jax.experimental.pallas import tpu as pltpu
from jax.sharding import PartitionSpec as P

MESH = pl.DeviceIdType.MESH
VMEM = pl.BlockSpec(memory_space=pltpu.VMEM)
ANY = pl.BlockSpec(memory_space=pl.ANY)
GROUP = 4


def flip(position):
    return position + (position // 2) * (1 - 2 * (position % 2))


def where_am_i():
    me = lax.axis_index("seq")
    return me // GROUP, me % GROUP


def device(plane, spot):
    return {"seq": plane * GROUP + spot}


def remote(source, target, sems, index, place):
    return pltpu.make_async_remote_copy(
        src_ref=source, dst_ref=target, send_sem=sems[0].at[index], recv_sem=sems[1].at[index],
        device_id=place, device_id_type=MESH,
    )


def greet(places):
    barrier = pltpu.get_barrier_semaphore()
    for place in places:
        pl.semaphore_signal(barrier, inc=1, device_id=place, device_id_type=MESH)
    pl.semaphore_wait(barrier, len(places))


class Ring:
    def __init__(self, own, slot, sems, base, mine, left, right, left_dev, right_dev):
        self.first = [
            remote(own(0), slot(mine, 0), sems, base, right_dev),
            remote(own(1), slot(mine, 1), sems, base + 1, left_dev),
            remote(own(1), slot(mine, 1), sems, base + 2, right_dev),
            remote(own(0), slot(mine, 0), sems, base + 3, left_dev),
        ]
        self.onward = [
            remote(slot(left, 0), slot(left, 0), sems, base + 4, right_dev),
            remote(slot(right, 1), slot(right, 1), sems, base + 5, left_dev),
        ]

    def start(self):
        for copy in self.first:
            copy.start()

    def relay(self):
        for arrived, onward in zip(self.first[:2], self.onward):
            arrived.wait_recv()
            onward.start()

    def finish(self):
        for copy in self.first[2:] + self.onward:
            copy.wait_recv()
        for copy in self.first + self.onward:
            copy.wait_send()


def rings():
    plane, spot = where_am_i()
    turn = flip(spot)
    left, right = flip((turn + GROUP - 1) % GROUP), flip((turn + 1) % GROUP)
    flat = (spot, left, right, device(plane, left), device(plane, right))
    below, above = (plane + GROUP - 1) % GROUP, (plane + 1) % GROUP
    tall = (plane, below, above, device(below, spot), device(above, spot))
    return plane, spot, flat, tall


def everyone(plane, spot, tall):
    return [device(plane, (spot + step) % GROUP) for step in range(1, GROUP)] + [tall[3], tall[4]]


def swap(piece, slot, sems, base, plane, spot):
    copies = []
    for step in range(1, GROUP):
        peer = (spot + step) % GROUP
        copies.append(remote(piece(peer), slot(spot), sems, base + step - 1, device(plane, peer)))
    return copies


def multiple(value, by):
    return pl.multiple_of(value, by)


def fetch_all(
    tok, pin, pout, key, query_tail, low_all, rows_all, key_all, query_edge,
    tok_all, pin_all, pieces, key_more, partial, inbox, low, send, recv, local,
):
    plane, spot, flat, tall = rings()
    core = lax.axis_index("ch")
    me, count = lax.axis_index("seq"), lax.axis_size("seq")
    sems = (send, recv)
    rows, ranks, width = tok.shape[0], pin.shape[0], pieces.shape[-1]
    margin = query_tail.shape[0]
    after, before = {"seq": (me + 1) % count}, {"seq": (me + count - 1) % count}
    partner = {"ch": 1 - core}
    greet(everyone(plane, spot, tall) + [partner, after, before])

    def columns(s, extent):
        return pl.ds(multiple(s * extent, extent), extent)

    half_tok, half_pin, half_low = rows // 2, ranks // 2, low.shape[0] // 2

    def low_rows(h):
        return pl.ds(multiple(margin + core * low.shape[0] + h * half_low, 16), half_low)

    tails = [
        remote(key.at[pl.ds(rows - margin, margin)], key_more.at[pl.ds(0, margin)], sems, 0, after),
        remote(query_tail, query_edge, sems, 1, after),
    ]
    rank_swap = swap(
        lambda peer: pout.at[:, columns(peer, width)], lambda s: pieces.at[s], sems, 2, plane, spot)
    key_swap = swap(
        lambda peer: key_more.at[:, columns(peer, width)], lambda s: key_all.at[s], sems, 5,
        plane, spot)
    tokens_ring = Ring(
        lambda h: tok.at[pl.ds(h * half_tok, half_tok)],
        lambda s, h: tok_all.at[s, pl.ds(h * half_tok, half_tok)], sems, 8, *flat)
    pin_ring = Ring(
        lambda h: pin.at[pl.ds(h * half_pin, half_pin)],
        lambda s, h: pin_all.at[pl.ds(multiple(s * ranks + h * half_pin, 16), half_pin)],
        sems, 14, *tall)
    rows_ring = Ring(
        lambda h: pieces.at[pl.ds(h * 2, 2)], lambda s, h: rows_all.at[pl.ds(h * 2, 2), s],
        sems, 20, *tall)
    low_ring = Ring(
        lambda h: low.at[pl.ds(h * half_low, half_low)],
        lambda s, h: low_all.at[low_rows(h), columns(s, low.shape[1])], sems, 26, *flat)
    mine = pl.ds(multiple(core * low.shape[0], 16), low.shape[0])
    others = pl.ds(multiple((1 - core) * low.shape[0], 16), low.shape[0])
    sums = remote(partial.at[others], inbox, sems, 32, partner)
    my_low = low_all.at[pl.ds(multiple(margin + core * low.shape[0], 16), low.shape[0])]
    lows = remote(my_low, my_low, sems, 33, partner)
    edge = remote(
        low_all.at[pl.ds(low_all.shape[0] - margin, margin)], low_all.at[pl.ds(0, margin)],
        sems, 34, tall[4])

    pin_ring.start()
    for copy in rank_swap + tails:
        copy.start()
    tokens_ring.start()
    keep = [
        pltpu.make_async_copy(tok, tok_all.at[spot], local.at[0]),
        pltpu.make_async_copy(pin, pin_all.at[columns(plane, ranks)], local.at[1]),
        pltpu.make_async_copy(pout.at[:, columns(spot, width)], pieces.at[spot], local.at[2]),
        pltpu.make_async_copy(key, key_more.at[pl.ds(margin, rows)], local.at[3]),
    ]
    for copy in keep:
        copy.start()
    for copy in keep:
        copy.wait()
    for copy in tails:
        copy.wait_recv()
    pin_ring.relay()
    for copy in rank_swap:
        copy.wait_recv()
    rows_ring.start()
    last = [
        pltpu.make_async_copy(pieces, rows_all.at[:, plane], local.at[4]),
        pltpu.make_async_copy(key_more.at[:, columns(spot, width)], key_all.at[spot], local.at[5]),
    ]
    for copy in last:
        copy.start()
    tokens_ring.relay()
    for copy in key_swap:
        copy.start()
    tokens_ring.finish()
    pin_ring.finish()

    @pl.loop(0, GROUP)
    def _(s):
        partial[pl.ds(multiple(s * rows, rows), rows), :] = lax.dot_general(
            tok_all[s], pin_all[...], (((1,), (1,)), ((), ())),
            preferred_element_type=jnp.float32)

    sums.start()
    sums.wait()
    low[...] = (partial[mine, :] + inbox[...]).astype(low.dtype)
    low_ring.start()
    keep_low = pltpu.make_async_copy(low, my_low.at[:, columns(spot, low.shape[1])], local.at[6])
    keep_low.start()
    low_ring.relay()
    rows_ring.relay()
    low_ring.finish()
    keep_low.wait()
    lows.start()
    lows.wait()
    edge.start()
    for copy in key_swap:
        copy.wait_recv()
    rows_ring.finish()
    edge.wait()
    for copy in rank_swap + key_swap + tails:
        copy.wait_send()
    for copy in last:
        copy.wait()


def share_states(mine, ends, send, recv, local):
    plane, spot = where_am_i()
    peers = [device((plane + step) % GROUP, spot) for step in range(1, GROUP)]
    greet(peers)
    copies = [
        remote(mine, ends.at[plane], (send, recv), index, peer) for index, peer in enumerate(peers)
    ]
    for copy in copies:
        copy.start()
    keep = pltpu.make_async_copy(mine, ends.at[plane], local.at[0])
    keep.start()
    for copy in copies:
        copy.wait()
    keep.wait()


def give_back(mine, out, send, recv, local):
    plane, spot = where_am_i()
    rows, width = out.shape[0], mine.shape[1]
    greet([device(plane, (spot + step) % GROUP) for step in range(1, GROUP)])

    def piece(peer):
        return mine.at[pl.ds(pl.multiple_of(peer * rows, rows), rows)]

    def slot(s):
        return out.at[:, pl.ds(pl.multiple_of(s * width, width), width)]

    moved = swap(piece, slot, (send, recv), 0, plane, spot)
    for copy in moved:
        copy.start()
    keep = pltpu.make_async_copy(piece(spot), slot(spot), local.at[0])
    keep.start()
    for copy in moved:
        copy.wait_recv()
    for copy in moved:
        copy.wait_send()
    keep.wait()


def talk(kernel, shapes, in_specs, scratch, copies, locals_, ident):
    one = not isinstance(shapes, (list, tuple))
    return pl.pallas_call(
        kernel,
        out_shape=shapes,
        in_specs=in_specs,
        out_specs=ANY if one else [ANY] * len(shapes),
        scratch_shapes=scratch + [
            pltpu.SemaphoreType.DMA((copies,)),
            pltpu.SemaphoreType.DMA((copies,)),
            pltpu.SemaphoreType.DMA((locals_,)),
        ],
        compiler_params=pltpu.CompilerParams(collective_id=ident, has_side_effects=True),
    )


def end_states(value, key, taps, decay, live, spread, states, values, keys):
    modes, tall, lanes = decay.shape
    margin = value.shape[0] - spread.shape[0] // tall
    count, rows = taps.shape[1], spread.shape[0] // tall
    piece = key.shape[1] - margin

    def lay(target, start, load):
        for column in range(tall):
            tile = load(slice(column * lanes, (column + 1) * lanes)).astype(jnp.float32)
            target[pl.ds(start * tall + column, 16, stride=tall), :] = tile

    @pl.loop(0, value.shape[0] // 16)
    def _(block):
        start = pl.multiple_of(block * 16, 16)
        lay(values, start, lambda cols: value[pl.ds(start, 16), cols])

    for edge in range(0, margin, 16):
        lay(keys, edge, lambda cols: key[0, edge:edge + 16, cols])
    for part in range(key.shape[0]):

        @pl.loop(0, piece // 16)
        def _(block):
            start = pl.multiple_of(block * 16, 16)
            lay(keys, margin + part * piece + start,
                lambda cols: key[part, pl.ds(margin + start, 16), cols])

    on = live[...]
    for row in range(margin):
        for target in (values, keys):
            place = slice(row * tall, (row + 1) * tall)
            target[place, :] = target[place, :] * on

    rates = [decay[mode] for mode in range(modes)]
    gains = [[taps[branch, tap] for tap in range(count)] for branch in range(2)]

    def short(source, gain, at):
        total = None
        for tap in range(count):
            place = pl.ds(pl.multiple_of((at + margin - tap) * tall, tall), tall)
            term = gain[tap] * source[place, :]
            total = term if total is None else total + term
        return total

    def step(at, held):
        for part in range(4):
            now = at * 4 + part
            mixed = short(keys, gains[0], now) * short(values, gains[1], now)
            mixed = mixed.astype(jnp.bfloat16).astype(jnp.float32)
            spread[pl.ds(pl.multiple_of(now * tall, tall), tall), :] = mixed
            held = [h * r + mixed for h, r in zip(held, rates)]
        return held

    held = lax.fori_loop(0, rows // 4, step, [jnp.zeros((tall, lanes), jnp.float32)] * modes)
    for mode in range(modes):
        states[mode] = held[mode]


def run_states(spread, ends, earlier, block, decay, weight, skip, out, kept):
    modes, tall, lanes = decay.shape
    rows = out.shape[0]
    rates = [decay[mode] for mode in range(modes)]
    weights = [weight[mode] for mode in range(modes)]
    gain = skip[...]

    def step(at, held):
        for part in range(4):
            place = pl.ds(pl.multiple_of((at * 4 + part) * tall, tall), tall)
            value = spread[place, :]
            held = [h * r + value for h, r in zip(held, rates)]
            terms = [h * w for h, w in zip(held, weights)]
            while len(terms) > 1:
                terms = [a + b for a, b in zip(terms[::2], terms[1::2])]
            rounded = terms[0].astype(jnp.bfloat16).astype(jnp.float32)
            kept[place, :] = rounded + gain * value
        return held

    carried = []
    for mode in range(modes):
        total = jnp.zeros((tall, lanes), jnp.float32)
        for at in range(ends.shape[0] - 1):
            total = jnp.where(earlier[at] > 0, total * block[mode] + ends[at, mode], total)
        carried.append(total)
    lax.fori_loop(0, rows // 4, step, carried)

    @pl.loop(0, rows // 16)
    def _(block):
        start = pl.multiple_of(block * 16, 16)
        for column in range(tall):
            tile = kept[pl.ds(start * tall + column, 16, stride=tall), :]
            out[pl.ds(start, 16), column * lanes:(column + 1) * lanes] = tile.astype(jnp.bfloat16)


def planes_device(
    tokens, query_in, key_in, proj_in, proj_out, short_taps, residues, mode_rates, skip_gain
):
    rows, channels = tokens.shape
    ranks = proj_in.shape[1]
    modes = residues.shape[0]
    margin_rows = short_taps.shape[1] - 1
    width, all_rows = channels // GROUP, rows * GROUP
    tall = width // 128
    half = jnp.bfloat16
    shape = jax.ShapeDtypeStruct
    plane, spot = where_am_i()
    margin = 16
    share, both = GROUP * ranks, GROUP * GROUP * ranks

    low_all, rows_all, key_all, query_edge = talk(
        fetch_all,
        [shape((margin + all_rows, both), half), shape((GROUP, GROUP, ranks, width), half),
         shape((GROUP, margin + rows, width), half), shape((margin, channels), half)],
        [VMEM] * 5,
        [pltpu.VMEM((GROUP, rows, channels), half), pltpu.VMEM((share, channels), half),
         pltpu.VMEM((GROUP, ranks, width), half), pltpu.VMEM((margin + rows, channels), half),
         pltpu.VMEM((all_rows, share), jnp.float32),
         pltpu.VMEM((all_rows // 2, share), jnp.float32), pltpu.VMEM((all_rows // 2, share), half)],
        35, 7, 1,
    )(tokens, proj_in.T, proj_out, key_in, query_in[rows - margin:])
    value = jnp.dot(
        low_all, rows_all.reshape(both, width), preferred_element_type=jnp.float32).astype(half)

    def mine(part):
        return lax.dynamic_slice_in_dim(part, spot * width, width, part.ndim - 1)

    tiles, tile = (modes, tall, 128), (tall, 128)
    rates, weights = mine(mode_rates), mine(residues)
    weights = (weights * jnp.sqrt(rates)).reshape(tiles)
    rates = rates.reshape(tiles)
    decay, block = jnp.exp(-rates), jnp.exp(-rates * all_rows)
    taps = mine(short_taps[1:]).reshape(2, margin_rows + 1, *tile)
    order = jnp.arange(GROUP - 1)[:, None, None]
    earlier = jnp.broadcast_to((order < plane).astype(jnp.float32), (GROUP - 1, *tile))
    scattered = pltpu.VMEM(((margin + all_rows) * tall, 128), jnp.float32)
    spread, states = pl.pallas_call(
        end_states,
        out_shape=[shape((all_rows * tall, 128), jnp.float32), shape(tiles, jnp.float32)],
        in_specs=[VMEM] * 5, out_specs=[VMEM] * 2, scratch_shapes=[scattered, scattered],
    )(value, key_all, taps, decay, earlier[0])
    ends = talk(share_states, shape((GROUP, *tiles), jnp.float32), [VMEM], [], 3, 1, 2)(states)
    mixed_out = pl.pallas_call(
        run_states,
        out_shape=shape((all_rows, width), half),
        in_specs=[VMEM] * 7, out_specs=VMEM,
        scratch_shapes=[pltpu.VMEM((all_rows * tall, 128), jnp.float32)],
    )(spread, ends, earlier, block, decay, weights, mine(skip_gain).reshape(tile))
    given = talk(give_back, shape((rows, channels), half), [VMEM], [], 3, 1, 3)(mixed_out)
    first = lax.axis_index("seq") == 0
    query_previous = jnp.where(first, 0, query_edge[margin - margin_rows:]).astype(half)
    query_short = short_filter(query_previous, query_in, short_taps[0])
    return (query_short * given.astype(jnp.float32)).astype(half)


precise = lax.Precision.HIGHEST


def carried_in(value, axis, join, neutral):
    count, mine = (lax.axis_size(axis), lax.axis_index(axis))
    pieces = jax.tree.map(lambda part: lax.all_gather(part, axis), value)
    total = jax.tree.map(
        lambda part, zero: jnp.full_like(part, 0) + jnp.asarray(zero, part.dtype), value, neutral
    )

    def turn(position, total):
        longer = join(total, jax.tree.map(lambda part: part[position], pieces))
        return jax.tree.map(lambda new, old: jnp.where(position < mine, new, old), longer, total)

    return lax.fori_loop(0, count - 1, turn, total)


def passed_along(value, axis, steps):
    count = lax.axis_size(axis)
    leading, last = (max(0, -steps), min(count, count - steps))
    return lax.ppermute(value, axis, [(source, source + steps) for source in range(leading, last)])


def short_filter(previous, current, filter_taps):
    margin_rows = filter_taps.shape[0] - 1
    length = current.shape[0]
    extended = jnp.concatenate([previous, current], axis=0).astype(jnp.float32)
    result = filter_taps[0] * extended[margin_rows : margin_rows + length]
    for offset in range(1, margin_rows + 1):
        result = (
            result
            + filter_taps[offset] * extended[margin_rows - offset : margin_rows - offset + length]
        )
    return result


def carry_states(earlier, later):
    return (earlier[0] * later[1] + later[0], earlier[1] * later[1])


def modal_convolve(mixed, residues, mode_rates):
    tok_rows = mixed.shape[0]
    signal = mixed.astype(jnp.float32)
    steps = jnp.arange(tok_rows, dtype=jnp.int32)
    lower = (steps[:, None] >= steps[None, :]).astype(jnp.float32)
    centred = (steps.astype(jnp.float32) - 0.5 * tok_rows)[:, None]
    local_total = jnp.zeros(signal.shape, jnp.float32)
    end_list = []
    for mode_index in range(residues.shape[0]):
        rate_mode = mode_rates[mode_index]
        weight = residues[mode_index] * jnp.sqrt(rate_mode)
        rising = jnp.exp(rate_mode * centred)
        falling = jnp.exp(-rate_mode * centred)
        running = falling * jnp.dot(lower, rising * signal, precision=precise)
        local_total = local_total + weight * running
        end_list.append(running[tok_rows - 1])
    end_states = jnp.stack(end_list)
    block_decay = jnp.exp(-mode_rates * tok_rows)
    identity = (jnp.zeros(end_states.shape, jnp.float32), jnp.ones(end_states.shape, jnp.float32))
    carried, _ = carried_in((end_states, block_decay), "seq", carry_states, identity)
    after = (steps.astype(jnp.float32) + 1.0)[:, None]
    for mode_index in range(residues.shape[0]):
        rate_mode = mode_rates[mode_index]
        weight = residues[mode_index] * jnp.sqrt(rate_mode)
        local_total = local_total + weight * carried[mode_index] * jnp.exp(-rate_mode * after)
    rounded = lax.optimization_barrier(local_total.astype(jnp.bfloat16))
    return rounded.astype(jnp.float32)


def per_device(
    tokens, query_in, key_in, proj_in, proj_out, short_taps, residues, mode_rates, skip_gain
):
    tok_rows = tokens.shape[0]
    margin_rows = short_taps.shape[1] - 1
    partial_value = jnp.dot(
        tokens,
        lax.all_gather(proj_in, "seq", axis=1, tiled=True),
        preferred_element_type=jnp.float32,
    )
    low_rank = lax.psum(partial_value, "ch").astype(jnp.bfloat16)
    value_full = jnp.dot(
        low_rank,
        lax.all_gather(proj_out, "seq", axis=0, tiled=True),
        preferred_element_type=jnp.float32,
    )
    value_proj = value_full.astype(jnp.bfloat16)
    edges = jnp.stack(
        [
            query_in[tok_rows - margin_rows :],
            key_in[tok_rows - margin_rows :],
            value_proj[tok_rows - margin_rows :],
        ]
    )
    arrived_edges = passed_along(edges, "seq", 1)
    query_previous = arrived_edges[0]
    key_previous = arrived_edges[1]
    value_previous = arrived_edges[2]
    query_short = short_filter(query_previous, query_in, short_taps[0])
    key_short = short_filter(key_previous, key_in, short_taps[1])
    value_short = short_filter(value_previous, value_proj, short_taps[2])
    mixed = (key_short * value_short).astype(jnp.bfloat16)
    convolved_tokens = modal_convolve(mixed, residues, mode_rates)
    return (query_short * (convolved_tokens + skip_gain * mixed.astype(jnp.float32))).astype(
        jnp.bfloat16
    )


def chosen(mesh):
    def run(*args):
        rows, channels = args[0].shape
        ranks = args[3].shape[1]
        square = mesh.shape["seq"] == GROUP * GROUP and mesh.shape["ch"] == 2
        whole = channels % (GROUP * 1024) == 0 and ranks % 32 == 0 and rows % 32 == 0
        fits = (GROUP * ranks) % 128 == 0 and channels == GROUP * 1024
        fits = fits and args[5].shape[1] <= 16
        return (planes_device if square and whole and fits else per_device)(*args)

    return run


def solution(mesh):
    placed = (
        P("seq", "ch"),
        P("seq", "ch"),
        P("seq", "ch"),
        P("ch", "seq"),
        P("seq", "ch"),
        P(None, None, "ch"),
        P(None, "ch"),
        P(None, "ch"),
        P("ch"),
    )
    return jax.shard_map(
        chosen(mesh), mesh=mesh, in_specs=placed, out_specs=P("seq", "ch"), check_vma=False
    )
```

```python
import functools

import jax
import jax.numpy as jnp
from jax import lax
from jax.experimental import pallas as pl
from jax.experimental.pallas import tpu as pltpu
from jax.sharding import PartitionSpec as P

MESH = pl.DeviceIdType.MESH
VMEM = pl.BlockSpec(memory_space=pltpu.VMEM)
ANY = pl.BlockSpec(memory_space=pl.ANY)
GROUP = 4


def flip(position):
    return position + (position // 2) * (1 - 2 * (position % 2))


def where_am_i():
    me = lax.axis_index("seq")
    return me // GROUP, me % GROUP


def device(plane, spot):
    return {"seq": plane * GROUP + spot}


def remote(source, target, sems, index, place):
    return pltpu.make_async_remote_copy(
        src_ref=source, dst_ref=target, send_sem=sems[0].at[index], recv_sem=sems[1].at[index],
        device_id=place, device_id_type=MESH,
    )


def greet(places):
    barrier = pltpu.get_barrier_semaphore()
    for place in places:
        pl.semaphore_signal(barrier, inc=1, device_id=place, device_id_type=MESH)
    pl.semaphore_wait(barrier, len(places))


class Ring:
    def __init__(self, own, slot, sems, base, mine, left, right, left_dev, right_dev):
        self.first = [
            remote(own(0), slot(mine, 0), sems, base, right_dev),
            remote(own(1), slot(mine, 1), sems, base + 1, left_dev),
            remote(own(1), slot(mine, 1), sems, base + 2, right_dev),
            remote(own(0), slot(mine, 0), sems, base + 3, left_dev),
        ]
        self.onward = [
            remote(slot(left, 0), slot(left, 0), sems, base + 4, right_dev),
            remote(slot(right, 1), slot(right, 1), sems, base + 5, left_dev),
        ]

    def start(self):
        for copy in self.first:
            copy.start()

    def relay(self):
        for arrived, onward in zip(self.first[:2], self.onward):
            arrived.wait_recv()
            onward.start()

    def finish(self):
        for copy in self.first[2:] + self.onward:
            copy.wait_recv()
        for copy in self.first + self.onward:
            copy.wait_send()


class Line:
    def __init__(self, own, slot, sems, base, plane, below, above, below_dev, above_dev):
        last = GROUP - 1

        def block(away):
            return slot((plane + away + GROUP) % GROUP)

        self.own, self.sent, self.arriving = [], [], []
        for step in range(last):
            for side, device_on, ahead in ((1, above_dev, plane < last), (-1, below_dev, plane > 0)):
                index = base + step + (0 if side > 0 else last)
                held = plane >= step if side > 0 else plane <= last - step
                due = plane >= step + 1 if side > 0 else plane <= last - step - 1
                out = remote(
                    own if step == 0 else block(-side * step), block(-side * step), sems, index,
                    device_on)
                came = block(-side * (step + 1))
                self.sent.append((ahead & held, out))
                self.arriving.append((due, remote(came, came, sems, index, device_on)))

    def start(self):
        for when, copy in self.sent[:2]:
            pl.when(when)(copy.start)

    def relay(self):
        for (due, arrived), (when, onward) in zip(self.arriving, self.sent[2:]):
            pl.when(due)(arrived.wait_recv)
            pl.when(when)(onward.start)

    def finish(self):
        for due, arrived in self.arriving[len(self.sent) - 2:]:
            pl.when(due)(arrived.wait_recv)
        for when, copy in self.sent:
            pl.when(when)(copy.wait_send)


def rings():
    plane, spot = where_am_i()
    turn = flip(spot)
    left, right = flip((turn + GROUP - 1) % GROUP), flip((turn + 1) % GROUP)
    flat = (spot, left, right, device(plane, left), device(plane, right))
    below, above = (plane + GROUP - 1) % GROUP, (plane + 1) % GROUP
    tall = (plane, below, above, device(below, spot), device(above, spot))
    return plane, spot, flat, tall


def everyone(plane, spot, tall):
    return [device(plane, (spot + step) % GROUP) for step in range(1, GROUP)] + [tall[3], tall[4]]


def swap(piece, slot, sems, base, plane, spot):
    copies = []
    for step in range(1, GROUP):
        peer = (spot + step) % GROUP
        copies.append(remote(piece(peer), slot(spot), sems, base + step - 1, device(plane, peer)))
    return copies


def multiple(value, by):
    return pl.multiple_of(value, by)


def fetch_all(
    tok, pin, pout, key, query, low_all, rows_all, key_all, query_edge,
    tok_all, pin_all, pieces, key_more, partial, inbox, low, send, recv, local,
):
    plane, spot, flat, tall = rings()
    core = lax.axis_index("ch")
    me, count = lax.axis_index("seq"), lax.axis_size("seq")
    sems = (send, recv)
    rows, ranks, width = tok.shape[0], pin.shape[0], pieces.shape[-1]
    margin = query_edge.shape[0]
    after, before = {"seq": (me + 1) % count}, {"seq": (me + count - 1) % count}
    partner = {"ch": 1 - core}
    greet(everyone(plane, spot, tall) + [partner, after, before])

    def columns(s, extent):
        return pl.ds(multiple(s * extent, extent), extent)

    half_tok, half_low = rows // 2, low.shape[0] // 2

    def low_rows(h):
        return pl.ds(multiple(margin + core * low.shape[0] + h * half_low, 16), half_low)

    tails = [
        remote(key.at[pl.ds(rows - margin, margin)], key_more.at[pl.ds(0, margin)], sems, 0, after),
        remote(query.at[pl.ds(rows - margin, margin)], query_edge, sems, 1, after),
    ]
    rank_swap = swap(
        lambda peer: pout.at[:, columns(peer, width)], lambda s: pieces.at[s], sems, 2, plane, spot)
    key_swap = swap(
        lambda peer: key_more.at[:, columns(peer, width)], lambda s: key_all.at[s], sems, 5,
        plane, spot)
    tokens_ring = Ring(
        lambda h: tok.at[pl.ds(h * half_tok, half_tok)],
        lambda s, h: tok_all.at[s, pl.ds(h * half_tok, half_tok)], sems, 8, *flat)
    pin_ring = Line(
        pin, lambda s: pin_all.at[columns(s, ranks)], sems, 14, *tall)
    rows_ring = Line(pieces, lambda s: rows_all.at[:, s], sems, 20, *tall)
    low_ring = Ring(
        lambda h: low.at[pl.ds(h * half_low, half_low)],
        lambda s, h: low_all.at[low_rows(h), columns(s, low.shape[1])], sems, 26, *flat)
    mine = pl.ds(multiple(core * low.shape[0], 16), low.shape[0])
    others = pl.ds(multiple((1 - core) * low.shape[0], 16), low.shape[0])
    sums = remote(partial.at[others], inbox, sems, 32, partner)
    my_low = low_all.at[pl.ds(multiple(margin + core * low.shape[0], 16), low.shape[0])]
    lows = remote(my_low, my_low, sems, 33, partner)
    edge = remote(
        low_all.at[pl.ds(low_all.shape[0] - margin, margin)], low_all.at[pl.ds(0, margin)],
        sems, 34, tall[4])

    pin_ring.start()
    for copy in rank_swap + tails:
        copy.start()
    tokens_ring.start()
    keep = [
        pltpu.make_async_copy(tok, tok_all.at[spot], local.at[0]),
        pltpu.make_async_copy(pin, pin_all.at[columns(plane, ranks)], local.at[1]),
        pltpu.make_async_copy(pout.at[:, columns(spot, width)], pieces.at[spot], local.at[2]),
        pltpu.make_async_copy(key, key_more.at[pl.ds(margin, rows)], local.at[3]),
    ]
    for copy in keep:
        copy.start()
    for copy in keep:
        copy.wait()
    for copy in tails:
        copy.wait_recv()
    pin_ring.relay()
    for copy in rank_swap:
        copy.wait_recv()
    rows_ring.start()
    last = [
        pltpu.make_async_copy(pieces, rows_all.at[:, plane], local.at[4]),
        pltpu.make_async_copy(key_more.at[:, columns(spot, width)], key_all.at[spot], local.at[5]),
    ]
    for copy in last:
        copy.start()
    tokens_ring.relay()
    for copy in key_swap:
        copy.start()
    tokens_ring.finish()
    pin_ring.finish()

    @pl.loop(0, GROUP)
    def _(s):
        partial[pl.ds(multiple(s * rows, rows), rows), :] = lax.dot_general(
            tok_all[s], pin_all[...], (((1,), (1,)), ((), ())),
            preferred_element_type=jnp.float32)

    sums.start()
    sums.wait()
    low[...] = (partial[mine, :] + inbox[...]).astype(low.dtype)
    low_ring.start()
    keep_low = pltpu.make_async_copy(low, my_low.at[:, columns(spot, low.shape[1])], local.at[6])
    keep_low.start()
    low_ring.relay()
    rows_ring.relay()
    low_ring.finish()
    keep_low.wait()
    lows.start()
    lows.wait()
    edge.start()
    for copy in key_swap:
        copy.wait_recv()
    rows_ring.finish()
    edge.wait()
    for copy in rank_swap + key_swap + tails:
        copy.wait_send()
    for copy in last:
        copy.wait()


def share_states(mine, ends, send, recv, local):
    plane, spot = where_am_i()
    peers = [device((plane + step) % GROUP, spot) for step in range(1, GROUP)]
    greet(peers)
    copies = [
        remote(mine, ends.at[plane], (send, recv), index, peer) for index, peer in enumerate(peers)
    ]
    for copy in copies:
        copy.start()
    keep = pltpu.make_async_copy(mine, ends.at[plane], local.at[0])
    keep.start()
    for copy in copies:
        copy.wait()
    keep.wait()


def give_back(mine, out, send, recv, local):
    plane, spot = where_am_i()
    rows, width = out.shape[0], mine.shape[1]
    greet([device(plane, (spot + step) % GROUP) for step in range(1, GROUP)])

    def piece(peer):
        return mine.at[pl.ds(pl.multiple_of(peer * rows, rows), rows)]

    def slot(s):
        return out.at[:, pl.ds(pl.multiple_of(s * width, width), width)]

    moved = swap(piece, slot, (send, recv), 0, plane, spot)
    for copy in moved:
        copy.start()
    keep = pltpu.make_async_copy(piece(spot), slot(spot), local.at[0])
    keep.start()
    for copy in moved:
        copy.wait_recv()
    for copy in moved:
        copy.wait_send()
    keep.wait()


def talk(kernel, shapes, in_specs, scratch, copies, locals_, ident):
    one = not isinstance(shapes, (list, tuple))
    return pl.pallas_call(
        kernel,
        out_shape=shapes,
        in_specs=in_specs,
        out_specs=ANY if one else [ANY] * len(shapes),
        scratch_shapes=scratch + [
            pltpu.SemaphoreType.DMA((copies,)),
            pltpu.SemaphoreType.DMA((copies,)),
            pltpu.SemaphoreType.DMA((locals_,)),
        ],
        compiler_params=pltpu.CompilerParams(collective_id=ident, has_side_effects=True),
    )


def end_states(value, key, taps, decay, live, spread, states, values, keys):
    modes, tall, lanes = decay.shape
    margin = value.shape[0] - spread.shape[0] // tall
    count, rows = taps.shape[1], spread.shape[0] // tall
    piece = key.shape[1] - margin

    def lay(target, start, load):
        for column in range(tall):
            tile = load(slice(column * lanes, (column + 1) * lanes)).astype(jnp.float32)
            target[pl.ds(start * tall + column, 16, stride=tall), :] = tile

    @pl.loop(0, value.shape[0] // 16)
    def _(block):
        start = pl.multiple_of(block * 16, 16)
        lay(values, start, lambda cols: value[pl.ds(start, 16), cols])

    for edge in range(0, margin, 16):
        lay(keys, edge, lambda cols: key[0, edge:edge + 16, cols])
    for part in range(key.shape[0]):

        @pl.loop(0, piece // 16)
        def _(block):
            start = pl.multiple_of(block * 16, 16)
            lay(keys, margin + part * piece + start,
                lambda cols: key[part, pl.ds(margin + start, 16), cols])

    on = live[...]
    for row in range(margin):
        for target in (values, keys):
            place = slice(row * tall, (row + 1) * tall)
            target[place, :] = target[place, :] * on

    rates = [decay[mode] for mode in range(modes)]
    gains = [[taps[branch, tap] for tap in range(count)] for branch in range(2)]

    def short(source, gain, at):
        total = None
        for tap in range(count):
            place = pl.ds(pl.multiple_of((at + margin - tap) * tall, tall), tall)
            term = gain[tap] * source[place, :]
            total = term if total is None else total + term
        return total

    def step(at, held):
        for part in range(4):
            now = at * 4 + part
            mixed = short(keys, gains[0], now) * short(values, gains[1], now)
            mixed = mixed.astype(jnp.bfloat16).astype(jnp.float32)
            spread[pl.ds(pl.multiple_of(now * tall, tall), tall), :] = mixed
            held = [h * r + mixed for h, r in zip(held, rates)]
        return held

    held = lax.fori_loop(0, rows // 4, step, [jnp.zeros((tall, lanes), jnp.float32)] * modes)
    for mode in range(modes):
        states[mode] = held[mode]


def run_states(spread, ends, earlier, block, decay, weight, skip, out, kept):
    modes, tall, lanes = decay.shape
    rows = out.shape[0]
    rates = [decay[mode] for mode in range(modes)]
    weights = [weight[mode] for mode in range(modes)]
    gain = skip[...]

    def step(at, held):
        for part in range(4):
            place = pl.ds(pl.multiple_of((at * 4 + part) * tall, tall), tall)
            value = spread[place, :]
            held = [h * r + value for h, r in zip(held, rates)]
            terms = [h * w for h, w in zip(held, weights)]
            while len(terms) > 1:
                terms = [a + b for a, b in zip(terms[::2], terms[1::2])]
            rounded = terms[0].astype(jnp.bfloat16).astype(jnp.float32)
            kept[place, :] = rounded + gain * value
        return held

    carried = []
    for mode in range(modes):
        total = jnp.zeros((tall, lanes), jnp.float32)
        for at in range(ends.shape[0] - 1):
            total = jnp.where(earlier[at] > 0, total * block[mode] + ends[at, mode], total)
        carried.append(total)
    lax.fori_loop(0, rows // 4, step, carried)

    @pl.loop(0, rows // 16)
    def _(block):
        start = pl.multiple_of(block * 16, 16)
        for column in range(tall):
            tile = kept[pl.ds(start * tall + column, 16, stride=tall), :]
            out[pl.ds(start, 16), column * lanes:(column + 1) * lanes] = tile.astype(jnp.bfloat16)


def planes_device(
    tokens, query_in, key_in, proj_in, proj_out, short_taps, residues, mode_rates, skip_gain
):
    rows, channels = tokens.shape
    ranks = proj_in.shape[1]
    modes = residues.shape[0]
    margin_rows = short_taps.shape[1] - 1
    width, all_rows = channels // GROUP, rows * GROUP
    tall = width // 128
    half = jnp.bfloat16
    shape = jax.ShapeDtypeStruct
    plane, spot = where_am_i()
    margin = 16
    share, both = GROUP * ranks, GROUP * GROUP * ranks

    low_all, rows_all, key_all, query_edge = talk(
        fetch_all,
        [shape((margin + all_rows, both), half), shape((GROUP, GROUP, ranks, width), half),
         shape((GROUP, margin + rows, width), half), shape((margin, channels), half)],
        [VMEM] * 4 + [ANY],
        [pltpu.VMEM((GROUP, rows, channels), half), pltpu.VMEM((share, channels), half),
         pltpu.VMEM((GROUP, ranks, width), half), pltpu.VMEM((margin + rows, channels), half),
         pltpu.VMEM((all_rows, share), jnp.float32),
         pltpu.VMEM((all_rows // 2, share), jnp.float32), pltpu.VMEM((all_rows // 2, share), half)],
        35, 7, 1,
    )(tokens, proj_in.T, proj_out, key_in, query_in)
    value = jnp.dot(
        low_all, rows_all.reshape(both, width), preferred_element_type=jnp.float32).astype(half)

    def mine(part):
        return lax.dynamic_slice_in_dim(part, spot * width, width, part.ndim - 1)

    tiles, tile = (modes, tall, 128), (tall, 128)
    rates, weights = mine(mode_rates), mine(residues)
    weights = (weights * jnp.sqrt(rates)).reshape(tiles)
    rates = rates.reshape(tiles)
    decay, block = jnp.exp(-rates), jnp.exp(-rates * all_rows)
    taps = mine(short_taps[1:]).reshape(2, margin_rows + 1, *tile)
    order = jnp.arange(GROUP - 1)[:, None, None]
    earlier = jnp.broadcast_to((order < plane).astype(jnp.float32), (GROUP - 1, *tile))
    scattered = pltpu.VMEM(((margin + all_rows) * tall, 128), jnp.float32)
    spread, states = pl.pallas_call(
        end_states,
        out_shape=[shape((all_rows * tall, 128), jnp.float32), shape(tiles, jnp.float32)],
        in_specs=[VMEM] * 5, out_specs=[VMEM] * 2, scratch_shapes=[scattered, scattered],
    )(value, key_all, taps, decay, earlier[0])
    ends = talk(share_states, shape((GROUP, *tiles), jnp.float32), [VMEM], [], 3, 1, 2)(states)
    mixed_out = pl.pallas_call(
        run_states,
        out_shape=shape((all_rows, width), half),
        in_specs=[VMEM] * 7, out_specs=VMEM,
        scratch_shapes=[pltpu.VMEM((all_rows * tall, 128), jnp.float32)],
    )(spread, ends, earlier, block, decay, weights, mine(skip_gain).reshape(tile))
    given = talk(give_back, shape((rows, channels), half), [VMEM], [], 3, 1, 3)(mixed_out)
    first = lax.axis_index("seq") == 0
    query_previous = jnp.where(first, 0, query_edge[margin - margin_rows:]).astype(half)
    query_short = short_filter(query_previous, query_in, short_taps[0])
    return (query_short * given.astype(jnp.float32)).astype(half)


precise = lax.Precision.HIGHEST


def carried_in(value, axis, join, neutral):
    count, mine = (lax.axis_size(axis), lax.axis_index(axis))
    pieces = jax.tree.map(lambda part: lax.all_gather(part, axis), value)
    total = jax.tree.map(
        lambda part, zero: jnp.full_like(part, 0) + jnp.asarray(zero, part.dtype), value, neutral
    )

    def turn(position, total):
        longer = join(total, jax.tree.map(lambda part: part[position], pieces))
        return jax.tree.map(lambda new, old: jnp.where(position < mine, new, old), longer, total)

    return lax.fori_loop(0, count - 1, turn, total)


def passed_along(value, axis, steps):
    count = lax.axis_size(axis)
    leading, last = (max(0, -steps), min(count, count - steps))
    return lax.ppermute(value, axis, [(source, source + steps) for source in range(leading, last)])


def short_filter(previous, current, filter_taps):
    margin_rows = filter_taps.shape[0] - 1
    length = current.shape[0]
    extended = jnp.concatenate([previous, current], axis=0).astype(jnp.float32)
    result = filter_taps[0] * extended[margin_rows : margin_rows + length]
    for offset in range(1, margin_rows + 1):
        result = (
            result
            + filter_taps[offset] * extended[margin_rows - offset : margin_rows - offset + length]
        )
    return result


def carry_states(earlier, later):
    return (earlier[0] * later[1] + later[0], earlier[1] * later[1])


def modal_convolve(mixed, residues, mode_rates):
    tok_rows = mixed.shape[0]
    signal = mixed.astype(jnp.float32)
    steps = jnp.arange(tok_rows, dtype=jnp.int32)
    lower = (steps[:, None] >= steps[None, :]).astype(jnp.float32)
    centred = (steps.astype(jnp.float32) - 0.5 * tok_rows)[:, None]
    local_total = jnp.zeros(signal.shape, jnp.float32)
    end_list = []
    for mode_index in range(residues.shape[0]):
        rate_mode = mode_rates[mode_index]
        weight = residues[mode_index] * jnp.sqrt(rate_mode)
        rising = jnp.exp(rate_mode * centred)
        falling = jnp.exp(-rate_mode * centred)
        running = falling * jnp.dot(lower, rising * signal, precision=precise)
        local_total = local_total + weight * running
        end_list.append(running[tok_rows - 1])
    end_states = jnp.stack(end_list)
    block_decay = jnp.exp(-mode_rates * tok_rows)
    identity = (jnp.zeros(end_states.shape, jnp.float32), jnp.ones(end_states.shape, jnp.float32))
    carried, _ = carried_in((end_states, block_decay), "seq", carry_states, identity)
    after = (steps.astype(jnp.float32) + 1.0)[:, None]
    for mode_index in range(residues.shape[0]):
        rate_mode = mode_rates[mode_index]
        weight = residues[mode_index] * jnp.sqrt(rate_mode)
        local_total = local_total + weight * carried[mode_index] * jnp.exp(-rate_mode * after)
    rounded = lax.optimization_barrier(local_total.astype(jnp.bfloat16))
    return rounded.astype(jnp.float32)


def per_device(
    tokens, query_in, key_in, proj_in, proj_out, short_taps, residues, mode_rates, skip_gain
):
    tok_rows = tokens.shape[0]
    margin_rows = short_taps.shape[1] - 1
    partial_value = jnp.dot(
        tokens,
        lax.all_gather(proj_in, "seq", axis=1, tiled=True),
        preferred_element_type=jnp.float32,
    )
    low_rank = lax.psum(partial_value, "ch").astype(jnp.bfloat16)
    value_full = jnp.dot(
        low_rank,
        lax.all_gather(proj_out, "seq", axis=0, tiled=True),
        preferred_element_type=jnp.float32,
    )
    value_proj = value_full.astype(jnp.bfloat16)
    edges = jnp.stack(
        [
            query_in[tok_rows - margin_rows :],
            key_in[tok_rows - margin_rows :],
            value_proj[tok_rows - margin_rows :],
        ]
    )
    arrived_edges = passed_along(edges, "seq", 1)
    query_previous = arrived_edges[0]
    key_previous = arrived_edges[1]
    value_previous = arrived_edges[2]
    query_short = short_filter(query_previous, query_in, short_taps[0])
    key_short = short_filter(key_previous, key_in, short_taps[1])
    value_short = short_filter(value_previous, value_proj, short_taps[2])
    mixed = (key_short * value_short).astype(jnp.bfloat16)
    convolved_tokens = modal_convolve(mixed, residues, mode_rates)
    return (query_short * (convolved_tokens + skip_gain * mixed.astype(jnp.float32))).astype(
        jnp.bfloat16
    )


def chosen(mesh):
    def run(*args):
        rows, channels = args[0].shape
        ranks = args[3].shape[1]
        square = mesh.shape["seq"] == GROUP * GROUP and mesh.shape["ch"] == 2
        whole = channels % (GROUP * 1024) == 0 and ranks % 32 == 0 and rows % 32 == 0
        fits = (GROUP * ranks) % 128 == 0 and channels == GROUP * 1024
        fits = fits and args[5].shape[1] <= 16
        return (planes_device if square and whole and fits else per_device)(*args)

    return run


def solution(mesh):
    placed = (
        P("seq", "ch"),
        P("seq", "ch"),
        P("seq", "ch"),
        P("ch", "seq"),
        P("seq", "ch"),
        P(None, None, "ch"),
        P(None, "ch"),
        P(None, "ch"),
        P("ch"),
    )
    return jax.shard_map(
        chosen(mesh), mesh=mesh, in_specs=placed, out_specs=P("seq", "ch"), check_vma=False
    )
```

```python
import functools

import jax
import jax.numpy as jnp
from jax import lax
from jax.experimental import pallas as pl
from jax.experimental.pallas import tpu as pltpu
from jax.sharding import PartitionSpec as P

MESH = pl.DeviceIdType.MESH
VMEM = pl.BlockSpec(memory_space=pltpu.VMEM)
ANY = pl.BlockSpec(memory_space=pl.ANY)
GROUP = 4


def flip(position):
    return position + (position // 2) * (1 - 2 * (position % 2))


def where_am_i():
    me = lax.axis_index("seq")
    return me // GROUP, me % GROUP


def device(plane, spot):
    return {"seq": plane * GROUP + spot}


def remote(source, target, sems, index, place):
    return pltpu.make_async_remote_copy(
        src_ref=source, dst_ref=target, send_sem=sems[0].at[index], recv_sem=sems[1].at[index],
        device_id=place, device_id_type=MESH,
    )


def greet(places):
    barrier = pltpu.get_barrier_semaphore()
    for place in places:
        pl.semaphore_signal(barrier, inc=1, device_id=place, device_id_type=MESH)
    pl.semaphore_wait(barrier, len(places))


class Ring:
    def __init__(self, own, slot, sems, base, mine, left, right, left_dev, right_dev):
        self.first = [
            remote(own(0), slot(mine, 0), sems, base, right_dev),
            remote(own(1), slot(mine, 1), sems, base + 1, left_dev),
            remote(own(1), slot(mine, 1), sems, base + 2, right_dev),
            remote(own(0), slot(mine, 0), sems, base + 3, left_dev),
        ]
        self.onward = [
            remote(slot(left, 0), slot(left, 0), sems, base + 4, right_dev),
            remote(slot(right, 1), slot(right, 1), sems, base + 5, left_dev),
        ]

    def start(self):
        for copy in self.first:
            copy.start()

    def relay(self):
        for arrived, onward in zip(self.first[:2], self.onward):
            arrived.wait_recv()
            onward.start()

    def finish(self):
        for copy in self.first[2:] + self.onward:
            copy.wait_recv()
        for copy in self.first + self.onward:
            copy.wait_send()


class Line:
    def __init__(self, own, slot, sems, base, plane, below, above, below_dev, above_dev):
        last = GROUP - 1

        def block(away):
            return slot((plane + away + GROUP) % GROUP)

        self.own, self.sent, self.arriving = [], [], []
        for step in range(last):
            for side, device_on, ahead in ((1, above_dev, plane < last), (-1, below_dev, plane > 0)):
                index = base + step + (0 if side > 0 else last)
                held = plane >= step if side > 0 else plane <= last - step
                due = plane >= step + 1 if side > 0 else plane <= last - step - 1
                out = remote(
                    own if step == 0 else block(-side * step), block(-side * step), sems, index,
                    device_on)
                came = block(-side * (step + 1))
                self.sent.append((ahead & held, out))
                self.arriving.append((due, remote(came, came, sems, index, device_on)))

    def start(self):
        for when, copy in self.sent[:2]:
            pl.when(when)(copy.start)

    def relay(self):
        for (due, arrived), (when, onward) in zip(self.arriving, self.sent[2:]):
            pl.when(due)(arrived.wait_recv)
            pl.when(when)(onward.start)

    def finish(self):
        for due, arrived in self.arriving[len(self.sent) - 2:]:
            pl.when(due)(arrived.wait_recv)
        for when, copy in self.sent:
            pl.when(when)(copy.wait_send)


def rings():
    plane, spot = where_am_i()
    turn = flip(spot)
    left, right = flip((turn + GROUP - 1) % GROUP), flip((turn + 1) % GROUP)
    flat = (spot, left, right, device(plane, left), device(plane, right))
    below, above = (plane + GROUP - 1) % GROUP, (plane + 1) % GROUP
    tall = (plane, below, above, device(below, spot), device(above, spot))
    return plane, spot, flat, tall


def everyone(plane, spot, tall):
    return [device(plane, (spot + step) % GROUP) for step in range(1, GROUP)] + [tall[3], tall[4]]


def swap(piece, slot, sems, base, plane, spot):
    copies = []
    for step in range(1, GROUP):
        peer = (spot + step) % GROUP
        copies.append(remote(piece(peer), slot(spot), sems, base + step - 1, device(plane, peer)))
    return copies


def multiple(value, by):
    return pl.multiple_of(value, by)


def fetch_all(
    tok, pin, pout, key, query, low_all, rows_all, key_all, query_edge,
    tok_all, pin_all, pieces, key_more, partial, inbox, low, send, recv, local,
):
    plane, spot, flat, tall = rings()
    core = lax.axis_index("ch")
    me, count = lax.axis_index("seq"), lax.axis_size("seq")
    sems = (send, recv)
    rows, ranks, width = tok.shape[0], pin.shape[0], pieces.shape[-1]
    margin = query_edge.shape[0]
    after, before = {"seq": (me + 1) % count}, {"seq": (me + count - 1) % count}
    partner = {"ch": 1 - core}
    greet(everyone(plane, spot, tall) + [partner, after, before])

    def columns(s, extent):
        return pl.ds(multiple(s * extent, extent), extent)

    half_tok, half_low = rows // 2, low.shape[0] // 2

    def low_rows(h):
        return pl.ds(multiple(margin + core * low.shape[0] + h * half_low, 16), half_low)

    tails = [
        remote(key.at[pl.ds(rows - margin, margin)], key_more.at[pl.ds(0, margin)], sems, 0, after),
        remote(query.at[pl.ds(rows - margin, margin)], query_edge, sems, 1, after),
    ]
    rank_swap = swap(
        lambda peer: pout.at[:, columns(peer, width)], lambda s: pieces.at[s], sems, 2, plane, spot)
    key_swap = swap(
        lambda peer: key_more.at[:, columns(peer, width)], lambda s: key_all.at[s], sems, 5,
        plane, spot)
    tokens_ring = Ring(
        lambda h: tok.at[pl.ds(h * half_tok, half_tok)],
        lambda s, h: tok_all.at[s, pl.ds(h * half_tok, half_tok)], sems, 8, *flat)
    pin_ring = Line(
        pin, lambda s: pin_all.at[columns(s, ranks)], sems, 14, *tall)
    rows_ring = Line(pieces, lambda s: rows_all.at[:, s], sems, 20, *tall)
    low_ring = Ring(
        lambda h: low.at[pl.ds(h * half_low, half_low)],
        lambda s, h: low_all.at[low_rows(h), columns(s, low.shape[1])], sems, 26, *flat)
    mine = pl.ds(multiple(core * low.shape[0], 16), low.shape[0])
    others = pl.ds(multiple((1 - core) * low.shape[0], 16), low.shape[0])
    sums = remote(partial.at[others], inbox, sems, 32, partner)
    my_low = low_all.at[pl.ds(multiple(margin + core * low.shape[0], 16), low.shape[0])]
    lows = remote(my_low, my_low, sems, 33, partner)
    edge = remote(
        low_all.at[pl.ds(low_all.shape[0] - margin, margin)], low_all.at[pl.ds(0, margin)],
        sems, 34, tall[4])

    pin_ring.start()
    for copy in rank_swap + tails:
        copy.start()
    tokens_ring.start()
    keep = [
        pltpu.make_async_copy(tok, tok_all.at[spot], local.at[0]),
        pltpu.make_async_copy(pin, pin_all.at[columns(plane, ranks)], local.at[1]),
        pltpu.make_async_copy(pout.at[:, columns(spot, width)], pieces.at[spot], local.at[2]),
        pltpu.make_async_copy(key, key_more.at[pl.ds(margin, rows)], local.at[3]),
    ]
    for copy in keep:
        copy.start()
    for copy in keep:
        copy.wait()
    for copy in tails:
        copy.wait_recv()
    pin_ring.relay()
    for copy in rank_swap:
        copy.wait_recv()
    rows_ring.start()
    last = [
        pltpu.make_async_copy(pieces, rows_all.at[:, plane], local.at[4]),
        pltpu.make_async_copy(key_more.at[:, columns(spot, width)], key_all.at[spot], local.at[5]),
    ]
    for copy in last:
        copy.start()
    tokens_ring.relay()
    for copy in key_swap:
        copy.start()
    tokens_ring.finish()
    pin_ring.finish()

    @pl.loop(0, GROUP)
    def _(s):
        partial[pl.ds(multiple(s * rows, rows), rows), :] = lax.dot_general(
            tok_all[s], pin_all[...], (((1,), (1,)), ((), ())),
            preferred_element_type=jnp.float32)

    sums.start()
    sums.wait()
    low[...] = (partial[mine, :] + inbox[...]).astype(low.dtype)
    low_ring.start()
    keep_low = pltpu.make_async_copy(low, my_low.at[:, columns(spot, low.shape[1])], local.at[6])
    keep_low.start()
    low_ring.relay()
    rows_ring.relay()
    low_ring.finish()
    keep_low.wait()
    lows.start()
    lows.wait()
    edge.start()
    for copy in key_swap:
        copy.wait_recv()
    rows_ring.finish()
    edge.wait()
    for copy in rank_swap + key_swap + tails:
        copy.wait_send()
    for copy in last:
        copy.wait()


def share_states(mine, ends, send, recv, local):
    plane, spot = where_am_i()
    peers = [device((plane + step) % GROUP, spot) for step in range(1, GROUP)]
    greet(peers)
    copies = [
        remote(mine, ends.at[plane], (send, recv), index, peer) for index, peer in enumerate(peers)
    ]
    for copy in copies:
        copy.start()
    keep = pltpu.make_async_copy(mine, ends.at[plane], local.at[0])
    keep.start()
    for copy in copies:
        copy.wait()
    keep.wait()


def give_back(mine, out, send, recv, local):
    plane, spot = where_am_i()
    rows, width = out.shape[0], mine.shape[1]
    greet([device(plane, (spot + step) % GROUP) for step in range(1, GROUP)])

    def piece(peer):
        return mine.at[pl.ds(pl.multiple_of(peer * rows, rows), rows)]

    def slot(s):
        return out.at[:, pl.ds(pl.multiple_of(s * width, width), width)]

    moved = swap(piece, slot, (send, recv), 0, plane, spot)
    for copy in moved:
        copy.start()
    keep = pltpu.make_async_copy(piece(spot), slot(spot), local.at[0])
    keep.start()
    for copy in moved:
        copy.wait_recv()
    for copy in moved:
        copy.wait_send()
    keep.wait()


def talk(kernel, shapes, in_specs, scratch, copies, locals_, ident):
    one = not isinstance(shapes, (list, tuple))
    return pl.pallas_call(
        kernel,
        out_shape=shapes,
        in_specs=in_specs,
        out_specs=ANY if one else [ANY] * len(shapes),
        scratch_shapes=scratch + [
            pltpu.SemaphoreType.DMA((copies,)),
            pltpu.SemaphoreType.DMA((copies,)),
            pltpu.SemaphoreType.DMA((locals_,)),
        ],
        compiler_params=pltpu.CompilerParams(collective_id=ident, has_side_effects=True),
    )


def tile_of(source, row, target, place):
    tall, lanes = target.shape[-2:]
    start = where_am_i()[1] * (tall * lanes)
    for column in range(tall):
        cols = pl.ds(pl.multiple_of(start + column * lanes, lanes), lanes)
        target[(*place, pl.ds(column, 1))] = source[(*row, cols)]


def end_states(
    value, key, all_taps, all_rates, spread, states, values, keys, taps, decay
):
    modes, tall, lanes = decay.shape
    for mode in range(modes):
        tile_of(all_rates, (pl.ds(mode, 1),), decay, (mode,))
        decay[mode] = jnp.exp(-decay[mode])
    for branch in range(2):
        for tap in range(taps.shape[1]):
            tile_of(all_taps, (branch + 1, pl.ds(tap, 1)), taps, (branch, tap))
    margin = value.shape[0] - spread.shape[0] // tall
    count, rows = taps.shape[1], spread.shape[0] // tall
    piece = key.shape[1] - margin

    def lay(target, start, load):
        for column in range(tall):
            tile = load(slice(column * lanes, (column + 1) * lanes)).astype(jnp.float32)
            target[pl.ds(start * tall + column, 16, stride=tall), :] = tile

    @pl.loop(0, value.shape[0] // 16)
    def _(block):
        start = pl.multiple_of(block * 16, 16)
        lay(values, start, lambda cols: value[pl.ds(start, 16), cols])

    for edge in range(0, margin, 16):
        lay(keys, edge, lambda cols: key[0, edge:edge + 16, cols])
    for part in range(key.shape[0]):

        @pl.loop(0, piece // 16)
        def _(block):
            start = pl.multiple_of(block * 16, 16)
            lay(keys, margin + part * piece + start,
                lambda cols: key[part, pl.ds(margin + start, 16), cols])

    on = (where_am_i()[0] > 0).astype(jnp.float32)
    for row in range(margin):
        for target in (values, keys):
            place = slice(row * tall, (row + 1) * tall)
            target[place, :] = target[place, :] * on

    rates = [decay[mode] for mode in range(modes)]
    gains = [[taps[branch, tap] for tap in range(count)] for branch in range(2)]

    def short(source, gain, at):
        total = None
        for tap in range(count):
            place = pl.ds(pl.multiple_of((at + margin - tap) * tall, tall), tall)
            term = gain[tap] * source[place, :]
            total = term if total is None else total + term
        return total

    def step(at, held):
        for part in range(4):
            now = at * 4 + part
            mixed = short(keys, gains[0], now) * short(values, gains[1], now)
            mixed = mixed.astype(jnp.bfloat16).astype(jnp.float32)
            spread[pl.ds(pl.multiple_of(now * tall, tall), tall), :] = mixed
            held = [h * r + mixed for h, r in zip(held, rates)]
        return held

    held = lax.fori_loop(0, rows // 4, step, [jnp.zeros((tall, lanes), jnp.float32)] * modes)
    for mode in range(modes):
        states[mode] = held[mode]


def run_states(spread, ends, all_rates, residues, skip, out, kept, rate, weight, gains):
    modes, tall, lanes = rate.shape
    rows = out.shape[0]
    plane = where_am_i()[0]
    for mode in range(modes):
        tile_of(all_rates, (pl.ds(mode, 1),), rate, (mode,))
        tile_of(residues, (pl.ds(mode, 1),), weight, (mode,))
    tile_of(skip, (pl.ds(0, 1),), gains, ())
    rates = [jnp.exp(-rate[mode]) for mode in range(modes)]
    weights = [weight[mode] * jnp.sqrt(rate[mode]) for mode in range(modes)]
    gain = gains[...]

    def step(at, held):
        for part in range(4):
            place = pl.ds(pl.multiple_of((at * 4 + part) * tall, tall), tall)
            value = spread[place, :]
            held = [h * r + value for h, r in zip(held, rates)]
            terms = [h * w for h, w in zip(held, weights)]
            while len(terms) > 1:
                terms = [a + b for a, b in zip(terms[::2], terms[1::2])]
            rounded = terms[0].astype(jnp.bfloat16).astype(jnp.float32)
            kept[place, :] = rounded + gain * value
        return held

    carried = []
    for mode in range(modes):
        total = jnp.zeros((tall, lanes), jnp.float32)
        for at in range(ends.shape[0] - 1):
            longer = total * jnp.exp(-rate[mode] * rows) + ends[at, mode]
            total = jnp.where(at < plane, longer, total)
        carried.append(total)
    lax.fori_loop(0, rows // 4, step, carried)

    @pl.loop(0, rows // 16)
    def _(block):
        start = pl.multiple_of(block * 16, 16)
        for column in range(tall):
            tile = kept[pl.ds(start * tall + column, 16, stride=tall), :]
            out[pl.ds(start, 16), column * lanes:(column + 1) * lanes] = tile.astype(jnp.bfloat16)


def planes_device(
    tokens, query_in, key_in, proj_in, proj_out, short_taps, residues, mode_rates, skip_gain
):
    rows, channels = tokens.shape
    ranks = proj_in.shape[1]
    modes = residues.shape[0]
    margin_rows = short_taps.shape[1] - 1
    width, all_rows = channels // GROUP, rows * GROUP
    tall = width // 128
    half = jnp.bfloat16
    shape = jax.ShapeDtypeStruct
    plane, spot = where_am_i()
    margin = 16
    share, both = GROUP * ranks, GROUP * GROUP * ranks

    low_all, rows_all, key_all, query_edge = talk(
        fetch_all,
        [shape((margin + all_rows, both), half), shape((GROUP, GROUP, ranks, width), half),
         shape((GROUP, margin + rows, width), half), shape((margin, channels), half)],
        [VMEM] * 4 + [ANY],
        [pltpu.VMEM((GROUP, rows, channels), half), pltpu.VMEM((share, channels), half),
         pltpu.VMEM((GROUP, ranks, width), half), pltpu.VMEM((margin + rows, channels), half),
         pltpu.VMEM((all_rows, share), jnp.float32),
         pltpu.VMEM((all_rows // 2, share), jnp.float32), pltpu.VMEM((all_rows // 2, share), half)],
        35, 7, 1,
    )(tokens, proj_in.T, proj_out, key_in, query_in)
    value = jnp.dot(
        low_all, rows_all.reshape(both, width), preferred_element_type=jnp.float32).astype(half)

    tiles, tile = (modes, tall, 128), (tall, 128)
    scattered = pltpu.VMEM(((margin + all_rows) * tall, 128), jnp.float32)
    spread, states = pl.pallas_call(
        end_states,
        out_shape=[shape((all_rows * tall, 128), jnp.float32), shape(tiles, jnp.float32)],
        in_specs=[VMEM] * 4, out_specs=[VMEM] * 2,
        scratch_shapes=[
            scattered, scattered, pltpu.VMEM((2, margin_rows + 1, *tile), jnp.float32),
            pltpu.VMEM(tiles, jnp.float32)],
    )(value, key_all, short_taps, mode_rates)
    ends = talk(share_states, shape((GROUP, *tiles), jnp.float32), [VMEM], [], 3, 1, 2)(states)
    mixed_out = pl.pallas_call(
        run_states,
        out_shape=shape((all_rows, width), half),
        in_specs=[VMEM] * 5, out_specs=VMEM,
        scratch_shapes=[
            pltpu.VMEM((all_rows * tall, 128), jnp.float32), pltpu.VMEM(tiles, jnp.float32),
            pltpu.VMEM(tiles, jnp.float32), pltpu.VMEM(tile, jnp.float32)],
    )(spread, ends, mode_rates, residues, skip_gain[None])
    given = talk(give_back, shape((rows, channels), half), [VMEM], [], 3, 1, 3)(mixed_out)
    first = lax.axis_index("seq") == 0
    query_previous = jnp.where(first, 0, query_edge[margin - margin_rows:]).astype(half)
    query_short = short_filter(query_previous, query_in, short_taps[0])
    return (query_short * given.astype(jnp.float32)).astype(half)


precise = lax.Precision.HIGHEST


def carried_in(value, axis, join, neutral):
    count, mine = (lax.axis_size(axis), lax.axis_index(axis))
    pieces = jax.tree.map(lambda part: lax.all_gather(part, axis), value)
    total = jax.tree.map(
        lambda part, zero: jnp.full_like(part, 0) + jnp.asarray(zero, part.dtype), value, neutral
    )

    def turn(position, total):
        longer = join(total, jax.tree.map(lambda part: part[position], pieces))
        return jax.tree.map(lambda new, old: jnp.where(position < mine, new, old), longer, total)

    return lax.fori_loop(0, count - 1, turn, total)


def passed_along(value, axis, steps):
    count = lax.axis_size(axis)
    leading, last = (max(0, -steps), min(count, count - steps))
    return lax.ppermute(value, axis, [(source, source + steps) for source in range(leading, last)])


def short_filter(previous, current, filter_taps):
    margin_rows = filter_taps.shape[0] - 1
    length = current.shape[0]
    extended = jnp.concatenate([previous, current], axis=0).astype(jnp.float32)
    result = filter_taps[0] * extended[margin_rows : margin_rows + length]
    for offset in range(1, margin_rows + 1):
        result = (
            result
            + filter_taps[offset] * extended[margin_rows - offset : margin_rows - offset + length]
        )
    return result


def carry_states(earlier, later):
    return (earlier[0] * later[1] + later[0], earlier[1] * later[1])


def modal_convolve(mixed, residues, mode_rates):
    tok_rows = mixed.shape[0]
    signal = mixed.astype(jnp.float32)
    steps = jnp.arange(tok_rows, dtype=jnp.int32)
    lower = (steps[:, None] >= steps[None, :]).astype(jnp.float32)
    centred = (steps.astype(jnp.float32) - 0.5 * tok_rows)[:, None]
    local_total = jnp.zeros(signal.shape, jnp.float32)
    end_list = []
    for mode_index in range(residues.shape[0]):
        rate_mode = mode_rates[mode_index]
        weight = residues[mode_index] * jnp.sqrt(rate_mode)
        rising = jnp.exp(rate_mode * centred)
        falling = jnp.exp(-rate_mode * centred)
        running = falling * jnp.dot(lower, rising * signal, precision=precise)
        local_total = local_total + weight * running
        end_list.append(running[tok_rows - 1])
    end_states = jnp.stack(end_list)
    block_decay = jnp.exp(-mode_rates * tok_rows)
    identity = (jnp.zeros(end_states.shape, jnp.float32), jnp.ones(end_states.shape, jnp.float32))
    carried, _ = carried_in((end_states, block_decay), "seq", carry_states, identity)
    after = (steps.astype(jnp.float32) + 1.0)[:, None]
    for mode_index in range(residues.shape[0]):
        rate_mode = mode_rates[mode_index]
        weight = residues[mode_index] * jnp.sqrt(rate_mode)
        local_total = local_total + weight * carried[mode_index] * jnp.exp(-rate_mode * after)
    rounded = lax.optimization_barrier(local_total.astype(jnp.bfloat16))
    return rounded.astype(jnp.float32)


def per_device(
    tokens, query_in, key_in, proj_in, proj_out, short_taps, residues, mode_rates, skip_gain
):
    tok_rows = tokens.shape[0]
    margin_rows = short_taps.shape[1] - 1
    partial_value = jnp.dot(
        tokens,
        lax.all_gather(proj_in, "seq", axis=1, tiled=True),
        preferred_element_type=jnp.float32,
    )
    low_rank = lax.psum(partial_value, "ch").astype(jnp.bfloat16)
    value_full = jnp.dot(
        low_rank,
        lax.all_gather(proj_out, "seq", axis=0, tiled=True),
        preferred_element_type=jnp.float32,
    )
    value_proj = value_full.astype(jnp.bfloat16)
    edges = jnp.stack(
        [
            query_in[tok_rows - margin_rows :],
            key_in[tok_rows - margin_rows :],
            value_proj[tok_rows - margin_rows :],
        ]
    )
    arrived_edges = passed_along(edges, "seq", 1)
    query_previous = arrived_edges[0]
    key_previous = arrived_edges[1]
    value_previous = arrived_edges[2]
    query_short = short_filter(query_previous, query_in, short_taps[0])
    key_short = short_filter(key_previous, key_in, short_taps[1])
    value_short = short_filter(value_previous, value_proj, short_taps[2])
    mixed = (key_short * value_short).astype(jnp.bfloat16)
    convolved_tokens = modal_convolve(mixed, residues, mode_rates)
    return (query_short * (convolved_tokens + skip_gain * mixed.astype(jnp.float32))).astype(
        jnp.bfloat16
    )


def chosen(mesh):
    def run(*args):
        rows, channels = args[0].shape
        ranks = args[3].shape[1]
        square = mesh.shape["seq"] == GROUP * GROUP and mesh.shape["ch"] == 2
        whole = channels % (GROUP * 1024) == 0 and ranks % 32 == 0 and rows % 32 == 0
        fits = (GROUP * ranks) % 128 == 0 and channels == GROUP * 1024
        fits = fits and args[5].shape[1] <= 16
        return (planes_device if square and whole and fits else per_device)(*args)

    return run


def solution(mesh):
    placed = (
        P("seq", "ch"),
        P("seq", "ch"),
        P("seq", "ch"),
        P("ch", "seq"),
        P("seq", "ch"),
        P(None, None, "ch"),
        P(None, "ch"),
        P(None, "ch"),
        P("ch"),
    )
    return jax.shard_map(
        chosen(mesh), mesh=mesh, in_specs=placed, out_specs=P("seq", "ch"), check_vma=False
    )
```
